32 devices in a mesh: scan: 8 (over z, y), grp: 4 (over x, core).
Axes of the slice: x: 2, y: 2, z: 4, core: 2. Of those that a mesh axis runs over, the one named last changes fastest.
Arguments:
- samples: float32 [128, 64, 6, 128], P('scan', 'grp'), may hold values from -6 to 6
- point_count: int32 [128], P('scan'), may hold values from 4096 to 8192
- corr_scan: int32 [128, 64], P('scan', 'grp'), may hold values from 0 to 127, as said below
- corr_tile: int32 [128, 64], P('scan', 'grp'), may hold values from 0 to 63
- corr_src: int32 [128, 64, 128], P('scan', 'grp'), may hold values from 0 to 2047
Outputs:
- hessian: float32 [128, 6, 6, 128], P('scan', None, None, 'grp')
- gradient: float32 [128, 6], P(('scan', 'grp'))
The draws below stay inside these ranges and needn't reach their ends.
Inputs may be any that keep to these rules, and one draw needn't show every extreme that they name: Never the scan of the entry's own row. A named tile is held by the device with scan index corr_scan // 16 and grp index corr_tile // 16; the 256 entries of one device name at most 16 tiles held by any one device, and in every draw some device is named exactly 16 times by every device.
All inputs are finite; a program needn't handle non-finite values.
Results may differ from the reference program's by a relative error of at most 0.00021.
Values sent between devices are 32-bit elements; how exact they have to be, the bound alone decides.
A program may use at most 64 MiB of HBM per device.

```python
import jax
import jax.numpy as jnp
from jax import lax

SCAN_LOC = 16
TILES_G = 16
CT = 16
SCANS = 128
TILES = 64
N_SCAN = 8
N_GRP = 4
DEVICES = 32


def pair_plan(key):
    half_count = DEVICES // 2
    slot_cap = 2 * SCAN_LOC * CT // DEVICES
    request_count = SCAN_LOC * CT
    hub_device = jax.random.randint(jax.random.fold_in(key, 1), (), 0, DEVICES)

    def one_device(device):
        dev_key = jax.random.fold_in(key, device + 100)

        def one_round(round_idx):
            round_key = jax.random.fold_in(dev_key, round_idx)
            shuffled = jax.random.permutation(round_key, DEVICES - 1) + 1
            offsets = jnp.concatenate([jnp.zeros((1,), jnp.int32), shuffled[:half_count - 1].astype(jnp.int32)])
            return (hub_device + offsets) % DEVICES
        destination = jax.vmap(one_round)(jnp.arange(slot_cap)).reshape(request_count)
        own_index = device // N_GRP
        dest_index = destination // N_GRP
        dest_group = destination % N_GRP
        local_scan = jnp.arange(request_count) // CT
        chosen = jax.random.randint(jax.random.fold_in(dev_key, 5000), (request_count,), 0, SCAN_LOC)
        clashes = (dest_index == own_index) & (chosen == local_scan)
        chosen = jnp.where(clashes, (chosen + 1) % SCAN_LOC, chosen)
        target_scan = dest_index * SCAN_LOC + chosen
        tile_ids = dest_group * TILES_G + jax.random.randint(jax.random.fold_in(dev_key, 6000), (request_count,), 0, TILES_G)
        return (target_scan.astype(jnp.int32), tile_ids.astype(jnp.int32))
    targets, tile_ids = jax.vmap(one_device)(jnp.arange(DEVICES))
    grid_shape = (N_SCAN, N_GRP, SCAN_LOC, CT)
    targets = targets.reshape(grid_shape).transpose(0, 2, 1, 3).reshape(N_SCAN * SCAN_LOC, N_GRP * CT)
    tile_ids = tile_ids.reshape(grid_shape).transpose(0, 2, 1, 3).reshape(N_SCAN * SCAN_LOC, N_GRP * CT)
    return (targets, tile_ids)


def draw_corr_scan(key, part):
    return pair_plan(key)[0]


def draw_corr_tile(key, part):
    return pair_plan(key)[1]


def set_ends(result, stream_key, smallest, top_value):
    longest = result.shape.index(max(result.shape))
    spots = []
    for shift in (0, 1):
        where = [jax.random.randint(jax.random.fold_in(stream_key, axis), (), 0, length) for axis, length in enumerate(result.shape)]
        where[longest] = (where[longest] + shift) % result.shape[longest]
        spots.append(tuple(where))
    return result.at[spots[0]].set(smallest).at[spots[1]].set(top_value)


def steps_of(own_key, extent, pieces, low, high):
    level, own = 1.0, jax.random.fold_in(own_key, 6)
    for dim, blocks in pieces:
        draws = jnp.exp(jax.random.uniform(jax.random.fold_in(own, dim), (blocks,), jnp.float32, low / len(pieces), high / len(pieces)))
        level = level * jnp.repeat(draws, extent[dim] // blocks).reshape([-1 if axis == dim else 1 for axis in range(len(extent))])
    return level


def scatter_about(key, shape, scale, limit, split=(), held_as=jnp.bfloat16):
    array = scale * jax.random.normal(key, shape, jnp.float32)
    if split:
        array = array * steps_of(key, shape, split, -0.22, 0.18)
    return jnp.clip(array, -limit, limit).astype(held_as)


def setup_inputs(seed: int = 0) -> dict:
    seeds = jax.random.split(jax.random.key(seed), 6)
    samples = scatter_about(seeds[0], (SCANS, TILES, 6, 128), 1.0, 6.0, ((0, 8), (1, 4)), jnp.float32)
    point_count = set_ends(jax.random.randint(seeds[1], (SCANS,), TILES_G * N_GRP * 64, TILES_G * N_GRP * 128 + 1), jax.random.fold_in(seeds[1], 1), TILES_G * N_GRP * 64, TILES_G * N_GRP * 128).astype(jnp.int32)
    corr_scan = draw_corr_scan(jax.random.fold_in(seeds[5], 71), 0)
    corr_tile = draw_corr_tile(jax.random.fold_in(seeds[5], 71), 0)
    corr_src = set_ends(jax.random.randint(seeds[4], (SCANS, N_GRP * CT, 128), 0, TILES_G * 128), jax.random.fold_in(seeds[4], 1), 0, (TILES_G * 128) - 1).astype(jnp.int32)
    return {"samples": samples, "point_count": point_count, "corr_scan": corr_scan, "corr_tile": corr_tile, "corr_src": corr_src}


def pair_blocks(pos_x, pos_y, pos_z, source_mask, tile_data):
    diff_x = pos_x - tile_data[:, 0, :]
    diff_y = pos_y - tile_data[:, 1, :]
    diff_z = pos_z - tile_data[:, 2, :]
    normal_x = tile_data[:, 3, :]
    normal_y = tile_data[:, 4, :]
    normal_z = tile_data[:, 5, :]
    residual = normal_x * diff_x + normal_y * diff_y + normal_z * diff_z
    weight = source_mask / (1.0 + residual * residual)
    jacobian = jnp.stack([pos_y * normal_z - pos_z * normal_y, pos_z * normal_x - pos_x * normal_z, pos_x * normal_y - pos_y * normal_x, normal_x, normal_y, normal_z], axis=1)
    blocks = jnp.einsum("nik,njk->nij", jacobian * weight[:, None, :], jacobian, precision=lax.Precision.HIGHEST)
    vectors = jnp.einsum("nik,nk->ni", jacobian, weight * residual, precision=lax.Precision.HIGHEST)
    return blocks.reshape(-1, 36), vectors


def reference(samples, point_count, corr_scan, corr_tile, corr_src):
    scan_count = samples.shape[0]
    tile_count = samples.shape[1]
    column_count = corr_scan.shape[1]
    per_group = column_count // N_GRP
    group_points = (tile_count // N_GRP) * 128
    groups = (jnp.arange(column_count) // per_group).astype(jnp.int32)
    point_ids = groups[None, :, None] * group_points + corr_src
    flat_samples = samples.reshape(scan_count, tile_count * 768)
    offsets = ((point_ids // 128) * 768 + point_ids % 128).reshape(scan_count, column_count * 128)
    coords = [jnp.take_along_axis(flat_samples, offsets + axis_id * 128, axis=1).reshape(-1, 128) for axis_id in range(3)]
    source_mask = (point_ids < point_count[:, None, None]).astype(jnp.float32).reshape(-1, 128)
    target_scan = corr_scan.reshape(-1)
    target_tile = corr_tile.reshape(-1)
    tile_data = samples[target_scan, target_tile]
    row_ids = jnp.arange(128).astype(jnp.int32)
    target_mask = ((target_tile[:, None] * 128 + row_ids[None, :]) < point_count[target_scan][:, None]).astype(jnp.float32)
    tile_data = jnp.concatenate([tile_data[:, 0:3, :], tile_data[:, 3:6, :] * target_mask[:, None, :]], axis=1)
    blocks, vectors = pair_blocks(coords[0], coords[1], coords[2], source_mask, tile_data)
    source_scan = (jnp.arange(scan_count * column_count) // column_count).astype(jnp.int32)
    pairwise = jnp.zeros((scan_count, scan_count, 36), jnp.float32)
    pairwise = pairwise.at[source_scan, source_scan].add(blocks)
    pairwise = pairwise.at[target_scan, target_scan].add(blocks)
    pairwise = pairwise.at[source_scan, target_scan].add(-blocks)
    pairwise = pairwise.at[target_scan, source_scan].add(-blocks)
    hessian = pairwise.reshape(scan_count, scan_count, 6, 6).transpose(0, 2, 3, 1)
    gradient = jnp.zeros((scan_count, 6), jnp.float32)
    gradient = gradient.at[source_scan].add(vectors).at[target_scan].add(-vectors)
    return hessian, gradient
```

```python
import functools

import jax
import jax.numpy as jnp
from jax import lax
from jax.experimental import pallas as pl
from jax.experimental.pallas import tpu as pltpu
from jax.sharding import PartitionSpec as P

LANES = 128
VALUES = 32
PAIRS = [(i, j) for i in range(6) for j in range(i, 6)]
VMEM = pl.BlockSpec(memory_space=pltpu.VMEM)
SMEM = pl.BlockSpec(memory_space=pltpu.SMEM)


def lane_take(table, index):
    return jnp.take_along_axis(table, index, axis=1, mode="promise_in_bounds")


def pack_kernel(cap, n_grp, samples, count, corr_scan, corr_tile, corr_src, data, meta, used):
    scan_local, tiles_local = samples.shape[0], samples.shape[1]
    per_scan = corr_src.shape[1]
    devices = meta.shape[0]
    scan_index, group_index = lax.axis_index("scan"), lax.axis_index("grp")
    first_point = group_index * tiles_local * LANES

    def clear(d, _):
        used[d] = 0
        for j in range(cap):
            meta[d, 0, j] = -1
            meta[d, 0, cap + j] = -1
        data[pl.ds(pl.multiple_of(d * cap * 4, 8), cap * 4), :] = jnp.zeros((cap * 4, LANES), jnp.float32)
        return 0

    lax.fori_loop(0, devices, clear, 0)

    def one_scan(s, _):
        wanted = corr_src[s]
        tile, lane = wanted >> 7, wanted & (LANES - 1)
        picked = [jnp.zeros((per_scan, LANES), jnp.float32)] * 3
        for t in range(tiles_local):
            hit = tile == t
            for c in range(3):
                row = jnp.broadcast_to(samples[s, t, pl.ds(c, 1), :], (per_scan, LANES))
                picked[c] = jnp.where(hit, lane_take(row, lane), picked[c])
        mask = jnp.where(first_point + wanted < count[s], 1.0, 0.0).astype(jnp.float32)
        picked.append(mask)
        for k in range(per_scan):
            b, t = corr_scan[s, k], corr_tile[s, k]
            d = b // scan_local * n_grp + t // tiles_local
            j = used[d]
            used[d] = j + 1
            meta[d, 0, j] = b % scan_local * tiles_local + t % tiles_local
            meta[d, 0, cap + j] = scan_index * scan_local + s
            base = (d * cap + j) * 4
            for c in range(4):
                data[pl.ds(base + c, 1), :] = picked[c][k : k + 1, :]
        return 0

    lax.fori_loop(0, scan_local, one_scan, 0)


def meet_all(n_grp, devices, me):
    barrier = pltpu.get_barrier_semaphore()

    def hello(k, _):
        peer = lax.rem(me + k, devices)
        pl.semaphore_signal(
            barrier, inc=1, device_id=(peer // n_grp, peer % n_grp), device_id_type=pl.DeviceIdType.MESH
        )
        return 0

    lax.fori_loop(1, devices, hello, 0)
    pl.semaphore_wait(barrier, devices - 1)


def remote(src, dst, send, recv, peer, n_grp):
    return pltpu.make_async_remote_copy(
        src_ref=src, dst_ref=dst, send_sem=send, recv_sem=recv,
        device_id=(peer // n_grp, peer % n_grp), device_id_type=pl.DeviceIdType.MESH,
    )


def swap_kernel(n_grp, rows, data, meta, data_in, meta_in, send_a, recv_a, send_b, recv_b, own):
    devices = meta.shape[0]
    me = lax.axis_index("scan") * n_grp + lax.axis_index("grp")

    def part(d):
        return pl.ds(pl.multiple_of(d * rows, rows), rows)

    meet_all(n_grp, devices, me)

    def start(k, _):
        peer = lax.rem(me + k, devices)
        remote(meta.at[peer], meta_in.at[me], send_b.at[peer], recv_b.at[me], peer, n_grp).start()
        remote(data.at[part(peer)], data_in.at[part(me)], send_a.at[peer], recv_a.at[me], peer, n_grp).start()
        return 0

    lax.fori_loop(1, devices, start, 0)
    local_a = pltpu.make_async_copy(data.at[part(me)], data_in.at[part(me)], own.at[0])
    local_b = pltpu.make_async_copy(meta.at[me], meta_in.at[me], own.at[1])
    local_a.start()
    local_b.start()
    local_a.wait()
    local_b.wait()

    def finish(k, _):
        peer = lax.rem(me + k, devices)
        a = remote(data.at[part(peer)], data_in.at[part(peer)], send_a.at[peer], recv_a.at[peer], peer, n_grp)
        b = remote(meta.at[peer], meta_in.at[peer], send_b.at[peer], recv_b.at[peer], peer, n_grp)
        a.wait_send()
        b.wait_send()
        a.wait_recv()
        b.wait_recv()
        return 0

    lax.fori_loop(1, devices, finish, 0)


def regroup(parts, width):
    groups = len(parts)
    lane = lax.broadcasted_iota(jnp.int32, parts[0].shape, 1) // width
    out = []
    for b in range(groups):
        total = parts[b]
        for g in range(groups):
            if g != b:
                total = jnp.where(lane == g, pltpu.roll(parts[g], (g - b) * width % LANES, 1), total)
        out.append(total)
    return out


def block_kernel(cap, n_grp, samples, count, meta, data, packed, tile_rows, scan_rows, sums):
    scan_local, tiles_local = samples.shape[0], samples.shape[1]
    n_scan, packed_rows = packed.shape[0], packed.shape[1]
    slots = n_scan * n_grp * cap
    width = n_grp * cap
    groups = LANES // width
    batch = 16
    scan_index, group_index = lax.axis_index("scan"), lax.axis_index("grp")
    lane = lax.broadcasted_iota(jnp.int32, (batch, LANES), 1)

    def one_batch(i, first):
        for j in range(batch):
            slot = first + i * batch + j
            d, place = slot // cap, slot % cap
            code = meta[d, 0, place]
            source = meta[d, 0, cap + place]
            safe = jnp.maximum(code, 0)
            b, t = safe // tiles_local, safe % tiles_local
            limit = count[b] - (group_index * tiles_local + t) * LANES
            partner = jnp.where(code < 0, -1, scan_index * scan_local + b)
            tile_rows[j * 8 : j * 8 + 6, :] = samples[b, t]
            tile_rows[j * 8 + 6 : j * 8 + 7, :] = jnp.full((1, LANES), limit.astype(jnp.float32))
            tile_rows[j * 8 + 7 : j * 8 + 8, :] = jnp.full((1, LANES), partner.astype(jnp.float32))
            scan_rows[j : j + 1, :] = jnp.full((1, LANES), source.astype(jnp.float32))
        rows = [tile_rows[pl.ds(c, batch, stride=8), :] for c in range(8)]
        base = (first + i * batch) * 4
        px, py, pz, mask = [data[pl.ds(base + c, batch, stride=4), :] for c in range(4)]
        valid = lane < rows[6].astype(jnp.int32)
        nx, ny, nz = [jnp.where(valid, rows[c], 0.0) for c in (3, 4, 5)]
        residual = nx * (px - rows[0]) + ny * (py - rows[1]) + nz * (pz - rows[2])
        weight = mask / (1.0 + residual * residual)
        jac = [py * nz - pz * ny, pz * nx - px * nz, px * ny - py * nx, nx, ny, nz]
        scaled = [weight * x for x in jac]
        products = [scaled[a] * jac[b] for a, b in PAIRS] + [x * residual for x in scaled]
        total = jnp.zeros((batch, LANES), jnp.float32)
        for q, product in enumerate(products):
            total = jnp.where(lane == q, jnp.sum(product, axis=1, keepdims=True), total)
        total = jnp.where(lane == 27, scan_rows[...], total)
        total = jnp.where(lane == 28, rows[7], total)
        sums[pl.ds(pl.multiple_of(i * batch, batch), batch), :] = total
        return first

    for c in range(slots // LANES):
        lax.fori_loop(0, LANES // batch, one_batch, c * LANES)
        turned = sums[...].T
        parts = [turned[g * packed_rows : (g + 1) * packed_rows, :] for g in range(groups)]
        for g, part in enumerate(regroup(parts, width)):
            packed[c * groups + g] = part


def share_kernel(n_grp, packed, by_source, by_partner, send_a, recv_a, send_b, recv_b, own):
    devices = by_source.shape[0]
    scan_index, group_index = lax.axis_index("scan"), lax.axis_index("grp")
    me = scan_index * n_grp + group_index
    meet_all(n_grp, devices, me)

    def whole(g):
        peer = scan_index * n_grp + g
        return remote(packed, by_partner.at[g], send_b.at[g], recv_b.at[g], peer, n_grp)

    for k in range(1, n_grp):
        g = lax.rem(group_index + k, n_grp)
        remote(
            packed, by_partner.at[group_index], send_b.at[g], recv_b.at[group_index], scan_index * n_grp + g, n_grp
        ).start()

    def start(k, _):
        peer = lax.rem(me + k, devices)
        remote(packed.at[peer // n_grp], by_source.at[me], send_a.at[peer], recv_a.at[me], peer, n_grp).start()
        return 0

    lax.fori_loop(1, devices, start, 0)
    local_a = pltpu.make_async_copy(packed.at[scan_index], by_source.at[me], own.at[0])
    local_b = pltpu.make_async_copy(packed, by_partner.at[group_index], own.at[1])
    local_a.start()
    local_b.start()
    local_a.wait()
    local_b.wait()

    def finish(k, _):
        peer = lax.rem(me + k, devices)
        a = remote(packed.at[peer // n_grp], by_source.at[peer], send_a.at[peer], recv_a.at[peer], peer, n_grp)
        a.wait_send()
        a.wait_recv()
        return 0

    lax.fori_loop(1, devices, finish, 0)
    for k in range(1, n_grp):
        b = whole(lax.rem(group_index + k, n_grp))
        b.wait_send()
        b.wait_recv()


def assemble_kernel(n_grp, width, by_source, by_partner, hessian, gradient, total):
    rows, columns = hessian.shape[0], hessian.shape[3]
    grad_rows = gradient.shape[0]
    packed_rows = by_source.shape[1]
    groups = LANES // width
    scan_index, group_index = lax.axis_index("scan"), lax.axis_index("grp")
    cells = rows * columns
    total[...] = jnp.zeros_like(total)
    step = 2 * groups

    def place(ids, first, size):
        local = ids - first
        return local, (local >= 0) & (local < size)

    def add(read, sign):
        def body(i, _):
            turned = []
            for half in range(2):
                parts = [read(i * step + half * groups + g) for g in range(groups)]
                turned.append(jnp.concatenate(regroup(parts, width), axis=0))
            values = jnp.concatenate(turned, axis=1)
            source, partner = values[27:28, :].astype(jnp.int32), values[28:29, :].astype(jnp.int32)
            own, other = (source, partner) if sign > 0 else (partner, source)
            row, row_ok = place(own, scan_index * rows, rows)
            plus, plus_ok = place(own, group_index * columns, columns)
            minus, minus_ok = place(other, group_index * columns, columns)
            plus = jnp.where(row_ok & plus_ok, row * columns + plus, -1)
            minus = jnp.where(row_ok & minus_ok, row * columns + minus, -1)
            grad, grad_ok = place(row, group_index * grad_rows, grad_rows)
            grad = jnp.where(row_ok & grad_ok, grad, -1)
            cell = lax.broadcasted_iota(jnp.int32, (cells, 2 * LANES), 0)
            chosen = jnp.where(cell == plus, 1.0, jnp.where(cell == minus, -1.0, 0.0))
            short = lax.broadcasted_iota(jnp.int32, (16, 2 * LANES), 0)
            chosen_grad = jnp.where(short == grad, float(sign), 0.0)
            matrix = jnp.concatenate([chosen, chosen_grad], axis=0).astype(jnp.bfloat16)
            high = values.astype(jnp.bfloat16)
            low = (values - high.astype(jnp.float32)).astype(jnp.bfloat16)
            both = jnp.concatenate([high, low], axis=0)
            total[...] += lax.dot_general(
                matrix, both, (((1,), (1,)), ((), ())), preferred_element_type=jnp.float32
            )
            return 0

        return body

    blocks = by_source.shape[0]
    n_scan = by_partner.shape[1]
    lax.fori_loop(0, blocks // step, add(lambda k: by_source[k], 1), 0)
    lax.fori_loop(0, blocks // step, add(lambda k: by_partner[k // n_scan, k % n_scan], -1), 0)
    result = total[:, 0:VALUES] + total[:, VALUES : 2 * VALUES]
    turned = result[0:cells, :].T
    where = {pair: q for q, pair in enumerate(PAIRS)}
    for i in range(6):
        ids = [where[min(i, j), max(i, j)] for j in range(6)]
        band = jnp.concatenate([turned[q : q + 1, :] for q in ids], axis=0)
        for r in range(rows):
            hessian[r, i] = band[:, r * columns : (r + 1) * columns]
    gradient[...] = result[cells : cells + grad_rows, 21:27]


def local(samples, point_count, corr_scan, corr_tile, corr_src):
    f32, i32 = jnp.float32, jnp.int32
    scan_local = samples.shape[0]
    request_count = scan_local * corr_scan.shape[1]
    n_scan, n_grp = lax.axis_size("scan"), lax.axis_size("grp")
    devices = n_scan * n_grp
    cap = 2 * request_count // devices
    width = n_grp * cap
    packed_rows = VALUES * width // LANES
    columns = scan_local * n_scan // n_grp
    grad_rows = scan_local // n_grp
    shape = jax.ShapeDtypeStruct
    dma = pltpu.SemaphoreType.DMA

    data, meta = pl.pallas_call(
        functools.partial(pack_kernel, cap, n_grp),
        out_shape=(shape((devices * cap * 4, LANES), f32), shape((devices, 1, LANES), i32)),
        in_specs=[VMEM, SMEM, SMEM, SMEM, VMEM],
        out_specs=(VMEM, SMEM),
        scratch_shapes=[pltpu.SMEM((devices,), i32)],
    )(samples, point_count, corr_scan, corr_tile, corr_src)

    data, meta = pl.pallas_call(
        functools.partial(swap_kernel, n_grp, cap * 4),
        out_shape=(shape(data.shape, f32), shape(meta.shape, i32)),
        in_specs=[VMEM, VMEM],
        out_specs=(VMEM, VMEM),
        scratch_shapes=[dma((devices,))] * 4 + [dma((2,))],
        compiler_params=pltpu.CompilerParams(collective_id=0, has_side_effects=True),
    )(data, meta)

    packed = pl.pallas_call(
        functools.partial(block_kernel, cap, n_grp),
        out_shape=shape((n_scan, packed_rows, LANES), f32),
        in_specs=[VMEM, SMEM, SMEM, VMEM],
        out_specs=VMEM,
        scratch_shapes=[
            pltpu.VMEM((LANES, LANES), f32),
            pltpu.VMEM((16, LANES), f32),
            pltpu.VMEM((LANES, LANES), f32),
        ],
    )(samples, point_count, meta, data)

    by_source, by_partner = pl.pallas_call(
        functools.partial(share_kernel, n_grp),
        out_shape=(
            shape((devices, packed_rows, LANES), f32),
            shape((n_grp, n_scan, packed_rows, LANES), f32),
        ),
        in_specs=[VMEM],
        out_specs=(VMEM, VMEM),
        scratch_shapes=[dma((devices,))] * 2 + [dma((n_grp,))] * 2 + [dma((2,))],
        compiler_params=pltpu.CompilerParams(collective_id=1, has_side_effects=True),
    )(packed)

    return pl.pallas_call(
        functools.partial(assemble_kernel, n_grp, width),
        out_shape=(shape((scan_local, 6, 6, columns), f32), shape((grad_rows, 6), f32)),
        in_specs=[VMEM, VMEM],
        out_specs=(VMEM, VMEM),
        scratch_shapes=[pltpu.VMEM((scan_local * columns + 16, 2 * VALUES), f32)],
    )(by_source, by_partner)


def solution(mesh):
    placed = (
        P("scan", "grp", None, None),
        P("scan"),
        P("scan", "grp"),
        P("scan", "grp"),
        P("scan", "grp", None),
    )
    return jax.shard_map(
        local,
        mesh=mesh,
        in_specs=placed,
        out_specs=(P("scan", None, None, "grp"), P(("scan", "grp"), None)),
        check_vma=False,
    )
```

```python
import functools

import jax
import jax.numpy as jnp
from jax import lax
from jax.experimental import pallas as pl
from jax.experimental.pallas import tpu as pltpu
from jax.sharding import PartitionSpec as P

LANES = 128
VALUES = 32
PAIRS = [(i, j) for i in range(6) for j in range(i, 6)]
VMEM = pl.BlockSpec(memory_space=pltpu.VMEM)
SMEM = pl.BlockSpec(memory_space=pltpu.SMEM)


def halves(value, size):
    if size & (size - 1):
        return value // size, value % size
    return value >> (size.bit_length() - 1), value & (size - 1)


def lane_take(table, index):
    return jnp.take_along_axis(table, index, axis=1, mode="promise_in_bounds")


def pack_kernel(cap, n_grp, samples, count, corr_scan, corr_tile, corr_src, data, meta, used):
    scan_local, tiles_local = samples.shape[0], samples.shape[2]
    per_scan = corr_src.shape[1]
    devices = meta.shape[0]
    scan_index, group_index = lax.axis_index("scan"), lax.axis_index("grp")
    first_point = group_index * tiles_local * LANES

    def clear(d, _):
        used[d] = 0
        for j in range(cap):
            meta[d, 0, j] = -1
            meta[d, 0, cap + j] = 0
            meta[d, 0, 2 * cap + j] = -1
        data[pl.ds(pl.multiple_of(d * cap * 4, 8), cap * 4), :] = jnp.zeros((cap * 4, LANES), jnp.float32)
        return 0

    lax.fori_loop(0, devices, clear, 0)

    def one_scan(s, _):
        wanted = corr_src[s]
        tile, lane = wanted >> 7, wanted & (LANES - 1)
        picked = [jnp.zeros((per_scan, LANES), jnp.float32)] * 3
        for t in range(tiles_local):
            hit = tile == t
            for c in range(3):
                row = jnp.broadcast_to(samples[s, c, pl.ds(t, 1), :], (per_scan, LANES))
                picked[c] = jnp.where(hit, lane_take(row, lane), picked[c])
        mask = jnp.where(first_point + wanted < count[s], 1.0, 0.0).astype(jnp.float32)
        picked.append(mask)
        for k in range(per_scan):
            b, t = corr_scan[s, k], corr_tile[s, k]
            (b_dev, b_loc), (t_dev, t_loc) = halves(b, scan_local), halves(t, tiles_local)
            d = b_dev * n_grp + t_dev
            j = used[d]
            used[d] = j + 1
            meta[d, 0, j] = b_loc
            meta[d, 0, cap + j] = t_loc
            meta[d, 0, 2 * cap + j] = scan_index * scan_local + s
            base = (d * cap + j) * 4
            for c in range(4):
                data[pl.ds(base + c, 1), :] = picked[c][k : k + 1, :]
        return 0

    lax.fori_loop(0, scan_local, one_scan, 0)


def meet_all(n_grp, devices, me):
    barrier = pltpu.get_barrier_semaphore()

    def hello(k, _):
        peer = lax.rem(me + k, devices)
        pl.semaphore_signal(
            barrier, inc=1, device_id=(peer // n_grp, peer % n_grp), device_id_type=pl.DeviceIdType.MESH
        )
        return 0

    lax.fori_loop(1, devices, hello, 0)
    pl.semaphore_wait(barrier, devices - 1)


def remote(src, dst, send, recv, peer, n_grp):
    return pltpu.make_async_remote_copy(
        src_ref=src, dst_ref=dst, send_sem=send, recv_sem=recv,
        device_id=(peer // n_grp, peer % n_grp), device_id_type=pl.DeviceIdType.MESH,
    )


def exchange_kernel(
    cap, n_grp, samples, count, data, meta, by_source, by_partner,
    data_in, meta_in, codes, comps, sums, packed,
    send_data, recv_data, send_meta, recv_meta, send_src, recv_src, send_part, recv_part, own,
):
    scan_local, tiles_local = samples.shape[0], samples.shape[2]
    n_scan, packed_rows = packed.shape[0], packed.shape[1]
    devices = n_scan * n_grp
    rows = cap * 4
    width = n_grp * cap
    groups = LANES // width
    batch = 16
    scan_index, group_index = lax.axis_index("scan"), lax.axis_index("grp")
    me = scan_index * n_grp + group_index
    lane = lax.broadcasted_iota(jnp.int32, (batch, LANES), 1)
    packed_lane = lax.broadcasted_iota(jnp.int32, (packed_rows, LANES), 1) // width

    def part(d):
        return pl.ds(pl.multiple_of(d * rows, rows), rows)

    def send_one(src, dst_index, send_index, recv_index, peer):
        return remote(
            data.at[part(src)], data_in.at[part(dst_index)], send_data.at[send_index], recv_data.at[recv_index], peer, n_grp
        )

    def send_code(src, dst_index, send_index, recv_index, peer):
        return remote(
            meta.at[src], meta_in.at[dst_index], send_meta.at[send_index], recv_meta.at[recv_index], peer, n_grp
        )

    def to_source(row, holder, peer, recv_index):
        return remote(packed.at[row], by_source.at[holder], send_src.at[peer], recv_src.at[recv_index], peer, n_grp)

    def to_partner(row, at, g):
        peer = scan_index * n_grp + g
        return remote(
            packed.at[row], by_partner.at[at, row], send_part.at[g, row], recv_part.at[at, row], peer, n_grp
        )

    meet_all(n_grp, devices, me)

    def start_meta(k, _):
        peer = lax.rem(me + k, devices)
        send_code(peer, me, peer, me, peer).start()
        return 0

    def start_data(k, _):
        peer = lax.rem(me + k, devices)
        send_one(peer, me, peer, me, peer).start()
        return 0

    def wait_meta(k, _):
        peer = lax.rem(me + k, devices)
        copy = send_code(peer, peer, peer, peer, peer)
        copy.wait_send()
        copy.wait_recv()
        return 0

    lax.fori_loop(1, devices, start_meta, 0)
    lax.fori_loop(1, devices, start_data, 0)
    own_data = pltpu.make_async_copy(data.at[part(me)], data_in.at[part(me)], own.at[0])
    own_meta = pltpu.make_async_copy(meta.at[me], meta_in.at[me], own.at[1])
    own_data.start()
    own_meta.start()
    sums[...] = jnp.zeros_like(sums)
    own_data.wait()
    own_meta.wait()
    lax.fori_loop(1, devices, wait_meta, 0)
    to_scalar = pltpu.make_async_copy(meta_in, codes, own.at[2])
    to_scalar.start()
    to_scalar.wait()

    def one_batch(i, row):
        for j in range(batch):
            step, place = halves(i * batch + j, cap)
            d = row * n_grp + step
            b, t = codes[d, 0, place], codes[d, 0, cap + place]
            source = codes[d, 0, 2 * cap + place]
            safe = jnp.maximum(b, 0)
            limit = count[safe] - (group_index * tiles_local + t) * LANES
            partner = jnp.where(b < 0, -1, scan_index * scan_local + b)
            for c in range(6):
                comps[c, j : j + 1, :] = samples[safe, c, pl.ds(t, 1), :]
            comps[6, j : j + 1, :] = jnp.full((1, LANES), limit.astype(jnp.float32))
            comps[7, j : j + 1, :] = jnp.full((1, LANES), partner.astype(jnp.float32))
            comps[8, j : j + 1, :] = jnp.full((1, LANES), source.astype(jnp.float32))
        base = (row * width + i * batch) * 4
        px, py, pz, mask = [data_in[pl.ds(base + c, batch, stride=4), :] for c in range(4)]
        valid = lane < comps[6].astype(jnp.int32)
        nx, ny, nz = [jnp.where(valid, comps[c], 0.0) for c in (3, 4, 5)]
        residual = nx * (px - comps[0]) + ny * (py - comps[1]) + nz * (pz - comps[2])
        weight = mask / (1.0 + residual * residual)
        jac = [py * nz - pz * ny, pz * nx - px * nz, px * ny - py * nx, nx, ny, nz]
        scaled = [weight * x for x in jac]
        products = [scaled[a] * jac[b] for a, b in PAIRS] + [x * residual for x in scaled]
        total = jnp.zeros((batch, LANES), jnp.float32)
        for q, product in enumerate(products):
            total = jnp.where(lane == q, jnp.sum(product, axis=1, keepdims=True), total)
        total = jnp.where(lane == 27, comps[8], total)
        total = jnp.where(lane == 28, comps[7], total)
        sums[pl.ds(pl.multiple_of(i * batch, batch), batch), :] = total
        return row

    def one_row(k, _):
        row = lax.rem(scan_index + n_scan - k, n_scan)
        for g in range(n_grp):
            source = row * n_grp + g

            @pl.when(source != me)
            def _():
                send_one(source, source, source, source, source).wait_recv()

        lax.fori_loop(0, width // batch, one_batch, row)
        turned = sums[...].T
        result = turned[0:packed_rows, :]
        for g in range(1, groups):
            moved = pltpu.roll(turned[g * packed_rows : (g + 1) * packed_rows, :], g * width, 1)
            result = jnp.where(packed_lane == g, moved, result)
        packed[row] = result
        by_partner[group_index, row] = result
        for g in range(n_grp):
            peer = row * n_grp + g

            @pl.when(peer != me)
            def _():
                to_source(row, me, peer, me).start()

        @pl.when(row == scan_index)
        def _():
            by_source[me] = result

        for g in range(1, n_grp):
            to_partner(row, group_index, lax.rem(group_index + g, n_grp)).start()
        return 0

    lax.fori_loop(0, n_scan, one_row, 0)

    def finish(k, _):
        peer = lax.rem(me + k, devices)
        send_one(peer, peer, peer, peer, peer).wait_send()
        copy = to_source(0, peer, peer, peer)
        copy.wait_send()
        copy.wait_recv()
        return 0

    lax.fori_loop(1, devices, finish, 0)

    def finish_partner(row, _):
        for k in range(1, n_grp):
            g = lax.rem(group_index + k, n_grp)
            copy = to_partner(row, g, g)
            copy.wait_send()
            copy.wait_recv()
        return 0

    lax.fori_loop(0, n_scan, finish_partner, 0)


def regroup(parts, width):
    groups = len(parts)
    lane = lax.broadcasted_iota(jnp.int32, parts[0].shape, 1) // width
    out = []
    for b in range(groups):
        total = parts[b]
        for g in range(groups):
            if g != b:
                total = jnp.where(lane == g, pltpu.roll(parts[g], (g - b) * width % LANES, 1), total)
        out.append(total)
    return out


def assemble_kernel(n_grp, width, by_source, by_partner, hessian, gradient, total):
    rows, columns = hessian.shape[2], hessian.shape[3]
    grad_rows = gradient.shape[0]
    packed_rows = by_source.shape[1]
    groups = LANES // width
    scan_index, group_index = lax.axis_index("scan"), lax.axis_index("grp")
    cells = rows * columns
    total[...] = jnp.zeros_like(total)
    step = 2 * groups

    def place(ids, first, size):
        local = ids - first
        return local, (local >= 0) & (local < size)

    def add(read, sign):
        def body(i, _):
            turned = []
            for half in range(2):
                parts = [read(i * step + half * groups + g) for g in range(groups)]
                turned.append(jnp.concatenate(regroup(parts, width), axis=0))
            values = jnp.concatenate(turned, axis=1)
            source, partner = values[27:28, :].astype(jnp.int32), values[28:29, :].astype(jnp.int32)
            own, other = (source, partner) if sign > 0 else (partner, source)
            row, row_ok = place(own, scan_index * rows, rows)
            plus, plus_ok = place(own, group_index * columns, columns)
            minus, minus_ok = place(other, group_index * columns, columns)
            plus = jnp.where(row_ok & plus_ok, row * columns + plus, -1)
            minus = jnp.where(row_ok & minus_ok, row * columns + minus, -1)
            grad, grad_ok = place(row, group_index * grad_rows, grad_rows)
            grad = jnp.where(row_ok & grad_ok, grad, -1)
            cell = lax.broadcasted_iota(jnp.int32, (cells, 2 * LANES), 0)
            chosen = jnp.where(cell == plus, 1.0, jnp.where(cell == minus, -1.0, 0.0))
            short = lax.broadcasted_iota(jnp.int32, (16, 2 * LANES), 0)
            chosen_grad = jnp.where(short == grad, float(sign), 0.0)
            matrix = jnp.concatenate([chosen, chosen_grad], axis=0).astype(jnp.bfloat16)
            high = values.astype(jnp.bfloat16)
            low = (values - high.astype(jnp.float32)).astype(jnp.bfloat16)
            both = jnp.concatenate([high, low], axis=0)
            total[...] += lax.dot_general(
                matrix, both, (((1,), (1,)), ((), ())), preferred_element_type=jnp.float32
            )
            return 0

        return body

    blocks = by_source.shape[0]
    n_scan = by_partner.shape[1]
    lax.fori_loop(0, blocks // step, add(lambda k: by_source[k], 1), 0)
    lax.fori_loop(0, blocks // step, add(lambda k: by_partner[k // n_scan, k % n_scan], -1), 0)
    result = total[:, 0:VALUES] + total[:, VALUES : 2 * VALUES]
    turned = result[0:cells, :].T
    where = {pair: q for q, pair in enumerate(PAIRS)}
    for i in range(6):
        ids = [where[min(i, j), max(i, j)] for j in range(6)]
        band = jnp.concatenate([turned[q : q + 1, :] for q in ids], axis=0)
        for r in range(rows):
            hessian[i, :, r, :] = band[:, r * columns : (r + 1) * columns]
    gradient[...] = result[cells : cells + grad_rows, 21:27]


def local(samples, point_count, corr_scan, corr_tile, corr_src):
    f32, i32 = jnp.float32, jnp.int32
    scan_local = samples.shape[0]
    request_count = scan_local * corr_scan.shape[1]
    n_scan, n_grp = lax.axis_size("scan"), lax.axis_size("grp")
    devices = n_scan * n_grp
    cap = 2 * request_count // devices
    width = n_grp * cap
    packed_rows = VALUES * width // LANES
    columns = scan_local * n_scan // n_grp
    grad_rows = scan_local // n_grp
    shape = jax.ShapeDtypeStruct
    dma = pltpu.SemaphoreType.DMA

    tiles = samples.transpose(0, 2, 1, 3)
    data, meta = pl.pallas_call(
        functools.partial(pack_kernel, cap, n_grp),
        out_shape=(shape((devices * cap * 4, LANES), f32), shape((devices, 1, LANES), i32)),
        in_specs=[VMEM, SMEM, SMEM, SMEM, VMEM],
        out_specs=(VMEM, SMEM),
        scratch_shapes=[pltpu.SMEM((devices,), i32)],
    )(tiles, point_count, corr_scan, corr_tile, corr_src)

    by_source, by_partner = pl.pallas_call(
        functools.partial(exchange_kernel, cap, n_grp),
        out_shape=(
            shape((devices, packed_rows, LANES), f32),
            shape((n_grp, n_scan, packed_rows, LANES), f32),
        ),
        in_specs=[VMEM, SMEM, VMEM, VMEM],
        out_specs=(VMEM, VMEM),
        scratch_shapes=[
            pltpu.VMEM(data.shape, f32),
            pltpu.VMEM(meta.shape, i32),
            pltpu.SMEM(meta.shape, i32),
            pltpu.VMEM((9, 16, LANES), f32),
            pltpu.VMEM((LANES, LANES), f32),
            pltpu.VMEM((n_scan, packed_rows, LANES), f32),
        ]
        + [dma((devices,))] * 6
        + [dma((n_grp, n_scan))] * 2
        + [dma((3,))],
        compiler_params=pltpu.CompilerParams(collective_id=0, has_side_effects=True),
    )(tiles, point_count, data, meta)

    hessian, gradient = pl.pallas_call(
        functools.partial(assemble_kernel, n_grp, width),
        out_shape=(shape((6, 6, scan_local, columns), f32), shape((grad_rows, 6), f32)),
        in_specs=[VMEM, VMEM],
        out_specs=(VMEM, VMEM),
        scratch_shapes=[pltpu.VMEM((scan_local * columns + 16, 2 * VALUES), f32)],
    )(by_source, by_partner)
    return hessian.transpose(2, 0, 1, 3), gradient


def solution(mesh):
    placed = (
        P("scan", "grp", None, None),
        P("scan"),
        P("scan", "grp"),
        P("scan", "grp"),
        P("scan", "grp", None),
    )
    return jax.shard_map(
        local,
        mesh=mesh,
        in_specs=placed,
        out_specs=(P("scan", None, None, "grp"), P(("scan", "grp"), None)),
        check_vma=False,
    )
```

```python
import functools

import jax
import jax.numpy as jnp
from jax import lax
from jax.experimental import pallas as pl
from jax.experimental.pallas import tpu as pltpu
from jax.sharding import PartitionSpec as P

LANES = 128
VALUES = 32
LEAST_POINTS = 4096
PAIRS = [(i, j) for i in range(6) for j in range(i, 6)]
VMEM = pl.BlockSpec(memory_space=pltpu.VMEM)
SMEM = pl.BlockSpec(memory_space=pltpu.SMEM)


def halves(value, size):
    if size & (size - 1):
        return value // size, value % size
    return value >> (size.bit_length() - 1), value & (size - 1)


def lane_take(table, index):
    return jnp.take_along_axis(table, index, axis=1, mode="promise_in_bounds")


def pack_kernel(cap, n_grp, samples, count, corr_scan, corr_tile, corr_src, data, meta, used):
    scan_local, tiles_local = samples.shape[0], samples.shape[2]
    per_scan = corr_src.shape[1]
    devices = meta.shape[0]
    scan_index, group_index = lax.axis_index("scan"), lax.axis_index("grp")
    first_point = group_index * tiles_local * LANES

    def clear(d, _):
        used[d] = 0
        for j in range(cap):
            meta[d, 0, j] = -1
            meta[d, 0, cap + j] = 0
            meta[d, 0, 2 * cap + j] = -1
        data[pl.ds(pl.multiple_of(d * cap * 4, 8), cap * 4), :] = jnp.zeros((cap * 4, LANES), jnp.float32)
        return 0

    lax.fori_loop(0, devices, clear, 0)

    def one_scan(s, _):
        wanted = corr_src[s]
        tile, lane = wanted >> 7, wanted & (LANES - 1)
        picked = [jnp.zeros((per_scan, LANES), jnp.float32)] * 3
        for t in range(tiles_local):
            hit = tile == t
            for c in range(3):
                row = jnp.broadcast_to(samples[s, c, pl.ds(t, 1), :], (per_scan, LANES))
                picked[c] = jnp.where(hit, lane_take(row, lane), picked[c])
        mask = jnp.where(first_point + wanted < count[s], 1.0, 0.0).astype(jnp.float32)
        picked.append(mask)
        for k in range(per_scan):
            b, t = corr_scan[s, k], corr_tile[s, k]
            (b_dev, b_loc), (t_dev, t_loc) = halves(b, scan_local), halves(t, tiles_local)
            d = b_dev * n_grp + t_dev
            j = used[d]
            used[d] = j + 1
            meta[d, 0, j] = b_loc
            meta[d, 0, cap + j] = t_loc
            meta[d, 0, 2 * cap + j] = scan_index * scan_local + s
            base = d * cap * 4 + j
            for c in range(4):
                data[pl.ds(base + c * cap, 1), :] = picked[c][k : k + 1, :]
        return 0

    lax.fori_loop(0, scan_local, one_scan, 0)


def meet_all(n_grp, devices, me):
    barrier = pltpu.get_barrier_semaphore()

    def hello(k, _):
        peer = lax.rem(me + k, devices)
        pl.semaphore_signal(
            barrier, inc=1, device_id=(peer // n_grp, peer % n_grp), device_id_type=pl.DeviceIdType.MESH
        )
        return 0

    lax.fori_loop(1, devices, hello, 0)
    pl.semaphore_wait(barrier, devices - 1)


def remote(src, dst, send, recv, peer, n_grp):
    return pltpu.make_async_remote_copy(
        src_ref=src, dst_ref=dst, send_sem=send, recv_sem=recv,
        device_id=(peer // n_grp, peer % n_grp), device_id_type=pl.DeviceIdType.MESH,
    )


def exchange_kernel(
    cap, n_grp, samples, count, data, meta, hessian, gradient,
    data_in, meta_in, codes, comps, sums, packed, by_source, by_partner, total_ref,
    send_data, recv_data, send_meta, recv_meta, send_src, recv_src, send_next, send_part, recv_part, own,
):
    scan_local, tiles_local = samples.shape[0], samples.shape[2]
    n_scan, packed_rows = packed.shape[0], packed.shape[1]
    devices = n_scan * n_grp
    rows = cap * 4
    width = n_grp * cap
    groups = LANES // width
    batch = 16
    scan_index, group_index = lax.axis_index("scan"), lax.axis_index("grp")
    me = scan_index * n_grp + group_index
    lane = lax.broadcasted_iota(jnp.int32, (batch, LANES), 1)
    packed_lane = lax.broadcasted_iota(jnp.int32, (packed_rows, LANES), 1) // width

    full_groups = min(LEAST_POINTS // (tiles_local * LANES), n_grp) if 3 * cap % 8 == 0 else 0
    short = rows - cap

    def send_one(src, dst_index, send_index, recv_index, peer, size):
        return remote(
            data.at[pl.ds(pl.multiple_of(src * rows, 8), size)],
            data_in.at[pl.ds(pl.multiple_of(dst_index * rows, 8), size)],
            send_data.at[send_index], recv_data.at[recv_index], peer, n_grp,
        )

    def send_code(src, dst_index, send_index, recv_index, peer):
        return remote(
            meta.at[src], meta_in.at[dst_index], send_meta.at[send_index], recv_meta.at[recv_index], peer, n_grp
        )

    def to_source(row, holder, peer, send_sem):
        return remote(packed.at[row], by_source.at[holder], send_sem, recv_src.at[holder], peer, n_grp)

    def hand_on(holder, g):
        return remote(
            by_source.at[holder], by_source.at[holder], send_next.at[g, holder // n_grp], recv_src.at[holder],
            scan_index * n_grp + g, n_grp,
        )

    def to_partner(row, at, g):
        peer = scan_index * n_grp + g
        return remote(
            packed.at[row], by_partner.at[at, row], send_part.at[g, row], recv_part.at[at, row], peer, n_grp
        )

    meet_all(n_grp, devices, me)

    def start_meta(k, _):
        peer = lax.rem(me + k, devices)
        send_code(peer, me, peer, me, peer).start()
        return 0

    def start_data(k, _):
        peer = lax.rem(me + k, devices)

        @pl.when(group_index < full_groups)
        def _():
            send_one(peer, me, peer, me, peer, short).start()

        @pl.when(group_index >= full_groups)
        def _():
            send_one(peer, me, peer, me, peer, rows).start()

        return 0

    def wait_meta(k, _):
        peer = lax.rem(me + k, devices)
        copy = send_code(peer, peer, peer, peer, peer)
        copy.wait_send()
        copy.wait_recv()
        return 0

    lax.fori_loop(1, devices, start_meta, 0)
    lax.fori_loop(1, devices, start_data, 0)
    own_data = pltpu.make_async_copy(
        data.at[pl.ds(pl.multiple_of(me * rows, 8), rows)], data_in.at[pl.ds(pl.multiple_of(me * rows, 8), rows)], own.at[0]
    )
    own_meta = pltpu.make_async_copy(meta.at[me], meta_in.at[me], own.at[1])
    own_data.start()
    own_meta.start()
    sums[...] = jnp.zeros_like(sums)
    own_data.wait()
    own_meta.wait()
    total_ref[...] = jnp.zeros_like(total_ref)

    def no_mask(row, _):
        for g in range(full_groups):
            first = pl.multiple_of((row * n_grp + g) * rows + short, 8)
            data_in[pl.ds(first, cap), :] = jnp.ones((cap, LANES), jnp.float32)
        return 0

    lax.fori_loop(0, n_scan, no_mask, 0)
    lax.fori_loop(1, devices, wait_meta, 0)
    to_scalar = pltpu.make_async_copy(meta_in, codes, own.at[2])
    to_scalar.start()
    to_scalar.wait()

    def one_batch(i, row):
        for j in range(batch):
            step, place = halves(i * batch + j, cap)
            d = row * n_grp + step
            b, t = codes[d, 0, place], codes[d, 0, cap + place]
            source = codes[d, 0, 2 * cap + place]
            safe = jnp.maximum(b, 0)
            limit = count[safe] - (group_index * tiles_local + t) * LANES
            partner = jnp.where(b < 0, -1, scan_index * scan_local + b)
            for c in range(6):
                comps[c, j : j + 1, :] = samples[safe, c, pl.ds(t, 1), :]
            comps[6, j : j + 1, :] = jnp.full((1, LANES), limit.astype(jnp.float32))
            comps[7, j : j + 1, :] = jnp.full((1, LANES), partner.astype(jnp.float32))
            comps[8, j : j + 1, :] = jnp.full((1, LANES), source.astype(jnp.float32))
        count_in = max(batch // cap, 1)
        read = []
        for c in range(4):
            pieces = []
            for piece in range(count_in):
                step, place = halves(i * batch + piece * cap, cap)
                base = (row * n_grp + step) * rows + c * cap + place
                pieces.append(data_in[pl.ds(base, min(batch, cap)), :])
            read.append(pieces[0] if count_in == 1 else jnp.concatenate(pieces, axis=0))
        px, py, pz, mask = read
        valid = lane < comps[6].astype(jnp.int32)
        nx, ny, nz = [jnp.where(valid, comps[c], 0.0) for c in (3, 4, 5)]
        residual = nx * (px - comps[0]) + ny * (py - comps[1]) + nz * (pz - comps[2])
        weight = mask / (1.0 + residual * residual)
        jac = [py * nz - pz * ny, pz * nx - px * nz, px * ny - py * nx, nx, ny, nz]
        scaled = [weight * x for x in jac]
        products = [scaled[a] * jac[b] for a, b in PAIRS] + [x * residual for x in scaled]
        total = jnp.zeros((batch, LANES), jnp.float32)
        for q, product in enumerate(products):
            total = jnp.where(lane == q, jnp.sum(product, axis=1, keepdims=True), total)
        total = jnp.where(lane == 27, comps[8], total)
        total = jnp.where(lane == 28, comps[7], total)
        sums[pl.ds(pl.multiple_of(i * batch, batch), batch), :] = total
        return row

    def one_row(k, _):
        row = lax.rem(scan_index + n_scan - k, n_scan)
        for g in range(n_grp):
            source = row * n_grp + g

            @pl.when(source != me)
            def _():
                send_one(source, source, source, source, source, short if g < full_groups else rows).wait_recv()

        lax.fori_loop(0, width // batch, one_batch, row)
        turned = sums[...].T
        result = turned[0:packed_rows, :]
        for g in range(1, groups):
            moved = pltpu.roll(turned[g * packed_rows : (g + 1) * packed_rows, :], g * width, 1)
            result = jnp.where(packed_lane == g, moved, result)
        packed[row] = result
        by_partner[group_index, row] = result
        for g in range(1, n_grp):
            to_partner(row, group_index, lax.rem(group_index + g, n_grp)).start()

        @pl.when(row != scan_index)
        def _():
            to_source(row, me, row * n_grp + group_index, send_src.at[row]).start()

        @pl.when(k >= lag)
        def _():
            add_partner(k - lag)

        return 0

    lag = 3
    rows_out, columns = hessian.shape[2], hessian.shape[3]
    grad_rows = gradient.shape[0]
    cells = rows_out * columns

    def add(blocks, sign):
        blocks = blocks + [jnp.zeros_like(blocks[0])] * (-n_grp % groups)
        turned = []
        for first in range(0, len(blocks), groups):
            turned.append(jnp.concatenate(regroup(blocks[first : first + groups], width), axis=0))
        values = jnp.concatenate(turned, axis=1)
        slots = values.shape[1]
        source, partner = values[27:28, :].astype(jnp.int32), values[28:29, :].astype(jnp.int32)
        mine, other = (source, partner) if sign > 0 else (partner, source)
        row = mine - scan_index * rows_out
        row_ok = (row >= 0) & (row < rows_out)
        plus, minus = mine - group_index * columns, other - group_index * columns
        plus = jnp.where(row_ok & (plus >= 0) & (plus < columns), row * columns + plus, -1)
        minus = jnp.where(row_ok & (minus >= 0) & (minus < columns), row * columns + minus, -1)
        grad = row - group_index * grad_rows
        grad = jnp.where(row_ok & (grad >= 0) & (grad < grad_rows), grad, -1)
        cell = lax.broadcasted_iota(jnp.int32, (cells, slots), 0)
        chosen = jnp.where(cell == plus, 1.0, jnp.where(cell == minus, -1.0, 0.0))
        few = lax.broadcasted_iota(jnp.int32, (16, slots), 0)
        chosen_grad = jnp.where(few == grad, float(sign), 0.0)
        matrix = jnp.concatenate([chosen, chosen_grad], axis=0).astype(jnp.bfloat16)
        high = values.astype(jnp.bfloat16)
        low = (values - high.astype(jnp.float32)).astype(jnp.bfloat16)
        both = jnp.concatenate([high, low], axis=0)
        total_ref[...] += lax.dot_general(
            matrix, both, (((1,), (1,)), ((), ())), preferred_element_type=jnp.float32
        )

    def add_partner(k):
        row = lax.rem(scan_index + n_scan - k, n_scan)
        for g in range(1, n_grp):
            at = lax.rem(group_index + g, n_grp)
            to_partner(row, at, at).wait_recv()
        add([by_partner[g, row] for g in range(n_grp)], -1)

    lax.fori_loop(0, n_scan, one_row, 0)

    def last_partner(k, _):
        add_partner(k)
        return 0

    lax.fori_loop(max(n_scan - lag, 0), n_scan, last_partner, 0)

    def pass_on(k, _):
        row = lax.rem(scan_index + k, n_scan)
        holder = row * n_grp + group_index
        to_source(row, holder, holder, send_src.at[row]).wait_recv()
        for g in range(1, n_grp):
            hand_on(holder, lax.rem(group_index + g, n_grp)).start()

        @pl.when(k > 1)
        def _():
            add_source(k - 1)

        return 0

    def add_source(k):
        row = lax.rem(scan_index + k, n_scan)
        for g in range(1, n_grp):
            holder = row * n_grp + lax.rem(group_index + g, n_grp)
            to_source(row, holder, holder, send_src.at[row]).wait_recv()
        add([by_source[row * n_grp + g] for g in range(n_grp)], 1)

    add([by_partner[g, scan_index] for g in range(n_grp)], 1)
    lax.fori_loop(1, n_scan, pass_on, 0)
    add_source(n_scan - 1)

    result = total_ref[:, 0:VALUES] + total_ref[:, VALUES : 2 * VALUES]
    turned = result[0:cells, :].T
    where = {pair: q for q, pair in enumerate(PAIRS)}
    for i in range(6):
        ids = [where[min(i, j), max(i, j)] for j in range(6)]
        band = jnp.concatenate([turned[q : q + 1, :] for q in ids], axis=0)
        for r in range(rows_out):
            hessian[i, :, r, :] = band[:, r * columns : (r + 1) * columns]
    gradient[...] = result[cells : cells + grad_rows, 21:27]

    def finish(k, _):
        peer = lax.rem(me + k, devices)

        @pl.when(group_index < full_groups)
        def _():
            send_one(peer, peer, peer, peer, peer, short).wait_send()

        @pl.when(group_index >= full_groups)
        def _():
            send_one(peer, peer, peer, peer, peer, rows).wait_send()

        return 0

    lax.fori_loop(1, devices, finish, 0)

    def finish_rows(k, _):
        row = lax.rem(scan_index + k, n_scan)
        for j in range(1, n_grp):
            to_partner(row, group_index, lax.rem(group_index + j, n_grp)).wait_send()

        @pl.when(k > 0)
        def _():
            to_source(row, me, row * n_grp + group_index, send_src.at[row]).wait_send()
            for j in range(1, n_grp):
                hand_on(row * n_grp + group_index, lax.rem(group_index + j, n_grp)).wait_send()

        return 0

    lax.fori_loop(0, n_scan, finish_rows, 0)


def regroup(parts, width):
    groups = len(parts)
    lane = lax.broadcasted_iota(jnp.int32, parts[0].shape, 1) // width
    out = []
    for b in range(groups):
        total = parts[b]
        for g in range(groups):
            if g != b:
                total = jnp.where(lane == g, pltpu.roll(parts[g], (g - b) * width % LANES, 1), total)
        out.append(total)
    return out


def local(samples, point_count, corr_scan, corr_tile, corr_src):
    f32, i32 = jnp.float32, jnp.int32
    scan_local = samples.shape[0]
    request_count = scan_local * corr_scan.shape[1]
    n_scan, n_grp = lax.axis_size("scan"), lax.axis_size("grp")
    devices = n_scan * n_grp
    cap = 2 * request_count // devices
    width = n_grp * cap
    packed_rows = VALUES * width // LANES
    columns = scan_local * n_scan // n_grp
    grad_rows = scan_local // n_grp
    shape = jax.ShapeDtypeStruct
    dma = pltpu.SemaphoreType.DMA

    tiles = samples.transpose(0, 2, 1, 3)
    data, meta = pl.pallas_call(
        functools.partial(pack_kernel, cap, n_grp),
        out_shape=(shape((devices * cap * 4, LANES), f32), shape((devices, 1, LANES), i32)),
        in_specs=[VMEM, SMEM, SMEM, SMEM, VMEM],
        out_specs=(VMEM, SMEM),
        scratch_shapes=[pltpu.SMEM((devices,), i32)],
    )(tiles, point_count, corr_scan, corr_tile, corr_src)

    hessian, gradient = pl.pallas_call(
        functools.partial(exchange_kernel, cap, n_grp),
        out_shape=(shape((6, 6, scan_local, columns), f32), shape((grad_rows, 6), f32)),
        in_specs=[VMEM, SMEM, VMEM, VMEM],
        out_specs=(VMEM, VMEM),
        scratch_shapes=[
            pltpu.VMEM(data.shape, f32),
            pltpu.VMEM(meta.shape, i32),
            pltpu.SMEM(meta.shape, i32),
            pltpu.VMEM((9, 16, LANES), f32),
            pltpu.VMEM((LANES, LANES), f32),
            pltpu.VMEM((n_scan, packed_rows, LANES), f32),
            pltpu.VMEM((devices, packed_rows, LANES), f32),
            pltpu.VMEM((n_grp, n_scan, packed_rows, LANES), f32),
            pltpu.VMEM((scan_local * columns + 16, 2 * VALUES), f32),
        ]
        + [dma((devices,))] * 4
        + [dma((n_scan,)), dma((devices,))]
        + [dma((n_grp, n_scan))] * 3
        + [dma((3,))],
        compiler_params=pltpu.CompilerParams(collective_id=0, has_side_effects=True),
    )(tiles, point_count, data, meta)
    return hessian.transpose(2, 0, 1, 3), gradient


def solution(mesh):
    placed = (
        P("scan", "grp", None, None),
        P("scan"),
        P("scan", "grp"),
        P("scan", "grp"),
        P("scan", "grp", None),
    )
    return jax.shard_map(
        local,
        mesh=mesh,
        in_specs=placed,
        out_specs=(P("scan", None, None, "grp"), P(("scan", "grp"), None)),
        check_vma=False,
    )
```

```python
import functools

import jax
import jax.numpy as jnp
from jax import lax
from jax.experimental import pallas as pl
from jax.experimental.pallas import tpu as pltpu
from jax.sharding import PartitionSpec as P

LANES = 128
VALUES = 32
LEAST_POINTS = 4096
PAIRS = [(i, j) for i in range(6) for j in range(i, 6)]
VMEM = pl.BlockSpec(memory_space=pltpu.VMEM)
SMEM = pl.BlockSpec(memory_space=pltpu.SMEM)


def halves(value, size):
    if size & (size - 1):
        return value // size, value % size
    return value >> (size.bit_length() - 1), value & (size - 1)


def lane_take(table, index):
    return jnp.take_along_axis(table, index, axis=1, mode="promise_in_bounds")


def pack_kernel(cap, n_grp, samples, count, corr_scan, corr_tile, corr_src, data, meta, used):
    scan_local, tiles_local = samples.shape[0], samples.shape[2]
    per_scan = corr_src.shape[1]
    devices = meta.shape[0]
    scan_index, group_index = lax.axis_index("scan"), lax.axis_index("grp")
    first_point = group_index * tiles_local * LANES

    def clear(d, _):
        used[d] = 0
        for j in range(cap):
            meta[d, 0, j] = -1
            meta[d, 0, cap + j] = 0
            meta[d, 0, 2 * cap + j] = -1
        data[pl.ds(pl.multiple_of(d * cap * 4, 8), cap * 4), :] = jnp.zeros((cap * 4, LANES), jnp.float32)
        return 0

    lax.fori_loop(0, devices, clear, 0)

    def one_scan(s, _):
        wanted = corr_src[s]
        tile, lane = wanted >> 7, wanted & (LANES - 1)
        picked = [jnp.zeros((per_scan, LANES), jnp.float32)] * 3
        for t in range(tiles_local):
            hit = tile == t
            for c in range(3):
                row = jnp.broadcast_to(samples[s, c, pl.ds(t, 1), :], (per_scan, LANES))
                picked[c] = jnp.where(hit, lane_take(row, lane), picked[c])
        mask = jnp.where(first_point + wanted < count[s], 1.0, 0.0).astype(jnp.float32)
        picked.append(mask)
        for k in range(per_scan):
            b, t = corr_scan[s, k], corr_tile[s, k]
            (b_dev, b_loc), (t_dev, t_loc) = halves(b, scan_local), halves(t, tiles_local)
            d = b_dev * n_grp + t_dev
            j = used[d]
            used[d] = j + 1
            meta[d, 0, j] = b_loc
            meta[d, 0, cap + j] = t_loc
            meta[d, 0, 2 * cap + j] = scan_index * scan_local + s
            base = d * cap * 4 + j
            for c in range(4):
                data[pl.ds(base + c * cap, 1), :] = picked[c][k : k + 1, :]
        return 0

    lax.fori_loop(0, scan_local, one_scan, 0)


def meet_all(n_grp, devices, me):
    barrier = pltpu.get_barrier_semaphore()

    def hello(k, _):
        peer = lax.rem(me + k, devices)
        pl.semaphore_signal(
            barrier, inc=1, device_id=(peer // n_grp, peer % n_grp), device_id_type=pl.DeviceIdType.MESH
        )
        return 0

    lax.fori_loop(1, devices, hello, 0)
    pl.semaphore_wait(barrier, devices - 1)


def remote(src, dst, send, recv, peer, n_grp):
    return pltpu.make_async_remote_copy(
        src_ref=src, dst_ref=dst, send_sem=send, recv_sem=recv,
        device_id=(peer // n_grp, peer % n_grp), device_id_type=pl.DeviceIdType.MESH,
    )


def exchange_kernel(
    cap, n_grp, samples, count, data, meta, by_source, by_partner,
    data_in, meta_in, codes, comps, sums, packed,
    send_data, recv_data, send_meta, recv_meta, send_src, recv_src, send_part, recv_part, own,
):
    scan_local, tiles_local = samples.shape[0], samples.shape[2]
    n_scan, packed_rows = packed.shape[0], packed.shape[1]
    devices = n_scan * n_grp
    rows = cap * 4
    width = n_grp * cap
    groups = LANES // width
    batch = 16
    scan_index, group_index = lax.axis_index("scan"), lax.axis_index("grp")
    me = scan_index * n_grp + group_index
    lane = lax.broadcasted_iota(jnp.int32, (batch, LANES), 1)
    packed_lane = lax.broadcasted_iota(jnp.int32, (packed_rows, LANES), 1) // width

    full_groups = min(LEAST_POINTS // (tiles_local * LANES), n_grp) if 3 * cap % 8 == 0 else 0
    short = rows - cap

    def send_one(src, dst_index, send_index, recv_index, peer, size):
        return remote(
            data.at[pl.ds(pl.multiple_of(src * rows, 8), size)],
            data_in.at[pl.ds(pl.multiple_of(dst_index * rows, 8), size)],
            send_data.at[send_index], recv_data.at[recv_index], peer, n_grp,
        )

    def send_code(src, dst_index, send_index, recv_index, peer):
        return remote(
            meta.at[src], meta_in.at[dst_index], send_meta.at[send_index], recv_meta.at[recv_index], peer, n_grp
        )

    def to_source(row, holder, peer, recv_index):
        return remote(packed.at[row], by_source.at[holder], send_src.at[peer], recv_src.at[recv_index], peer, n_grp)

    def to_partner(row, at, g):
        peer = scan_index * n_grp + g
        return remote(
            packed.at[row], by_partner.at[at, row], send_part.at[g, row], recv_part.at[at, row], peer, n_grp
        )

    meet_all(n_grp, devices, me)

    def start_meta(k, _):
        peer = lax.rem(me + k, devices)
        send_code(peer, me, peer, me, peer).start()
        return 0

    def start_data(k, _):
        peer = lax.rem(me + k, devices)

        @pl.when(group_index < full_groups)
        def _():
            send_one(peer, me, peer, me, peer, short).start()

        @pl.when(group_index >= full_groups)
        def _():
            send_one(peer, me, peer, me, peer, rows).start()

        return 0

    def wait_meta(k, _):
        peer = lax.rem(me + k, devices)
        copy = send_code(peer, peer, peer, peer, peer)
        copy.wait_send()
        copy.wait_recv()
        return 0

    lax.fori_loop(1, devices, start_meta, 0)
    lax.fori_loop(1, devices, start_data, 0)
    own_data = pltpu.make_async_copy(
        data.at[pl.ds(pl.multiple_of(me * rows, 8), rows)], data_in.at[pl.ds(pl.multiple_of(me * rows, 8), rows)], own.at[0]
    )
    own_meta = pltpu.make_async_copy(meta.at[me], meta_in.at[me], own.at[1])
    own_data.start()
    own_meta.start()
    sums[...] = jnp.zeros_like(sums)
    own_data.wait()
    own_meta.wait()

    def no_mask(row, _):
        for g in range(full_groups):
            first = pl.multiple_of((row * n_grp + g) * rows + short, 8)
            data_in[pl.ds(first, cap), :] = jnp.ones((cap, LANES), jnp.float32)
        return 0

    lax.fori_loop(0, n_scan, no_mask, 0)
    lax.fori_loop(1, devices, wait_meta, 0)
    to_scalar = pltpu.make_async_copy(meta_in, codes, own.at[2])
    to_scalar.start()
    to_scalar.wait()

    def one_batch(i, row):
        for j in range(batch):
            step, place = halves(i * batch + j, cap)
            d = row * n_grp + step
            b, t = codes[d, 0, place], codes[d, 0, cap + place]
            source = codes[d, 0, 2 * cap + place]
            safe = jnp.maximum(b, 0)
            limit = count[safe] - (group_index * tiles_local + t) * LANES
            partner = jnp.where(b < 0, -1, scan_index * scan_local + b)
            for c in range(6):
                comps[c, j : j + 1, :] = samples[safe, c, pl.ds(t, 1), :]
            comps[6, j : j + 1, :] = jnp.full((1, LANES), limit.astype(jnp.float32))
            comps[7, j : j + 1, :] = jnp.full((1, LANES), partner.astype(jnp.float32))
            comps[8, j : j + 1, :] = jnp.full((1, LANES), source.astype(jnp.float32))
        count_in = max(batch // cap, 1)
        read = []
        for c in range(4):
            pieces = []
            for piece in range(count_in):
                step, place = halves(i * batch + piece * cap, cap)
                base = (row * n_grp + step) * rows + c * cap + place
                pieces.append(data_in[pl.ds(base, min(batch, cap)), :])
            read.append(pieces[0] if count_in == 1 else jnp.concatenate(pieces, axis=0))
        px, py, pz, mask = read
        valid = lane < comps[6].astype(jnp.int32)
        nx, ny, nz = [jnp.where(valid, comps[c], 0.0) for c in (3, 4, 5)]
        residual = nx * (px - comps[0]) + ny * (py - comps[1]) + nz * (pz - comps[2])
        weight = mask / (1.0 + residual * residual)
        jac = [py * nz - pz * ny, pz * nx - px * nz, px * ny - py * nx, nx, ny, nz]
        scaled = [weight * x for x in jac]
        products = [scaled[a] * jac[b] for a, b in PAIRS] + [x * residual for x in scaled]
        total = jnp.zeros((batch, LANES), jnp.float32)
        for q, product in enumerate(products):
            total = jnp.where(lane == q, jnp.sum(product, axis=1, keepdims=True), total)
        total = jnp.where(lane == 27, comps[8], total)
        total = jnp.where(lane == 28, comps[7], total)
        sums[pl.ds(pl.multiple_of(i * batch, batch), batch), :] = total
        return row

    def one_row(k, _):
        row = lax.rem(scan_index + n_scan - k, n_scan)
        for g in range(n_grp):
            source = row * n_grp + g

            @pl.when(source != me)
            def _():
                send_one(source, source, source, source, source, short if g < full_groups else rows).wait_recv()

        lax.fori_loop(0, width // batch, one_batch, row)
        turned = sums[...].T
        result = turned[0:packed_rows, :]
        for g in range(1, groups):
            moved = pltpu.roll(turned[g * packed_rows : (g + 1) * packed_rows, :], g * width, 1)
            result = jnp.where(packed_lane == g, moved, result)
        packed[row] = result
        by_partner[group_index, row] = result
        for g in range(n_grp):
            peer = row * n_grp + g

            @pl.when(peer != me)
            def _():
                to_source(row, me, peer, me).start()

        @pl.when(row == scan_index)
        def _():
            by_source[me] = result

        for g in range(1, n_grp):
            to_partner(row, group_index, lax.rem(group_index + g, n_grp)).start()
        return 0

    lax.fori_loop(0, n_scan, one_row, 0)

    def finish(k, _):
        peer = lax.rem(me + k, devices)

        @pl.when(group_index < full_groups)
        def _():
            send_one(peer, peer, peer, peer, peer, short).wait_send()

        @pl.when(group_index >= full_groups)
        def _():
            send_one(peer, peer, peer, peer, peer, rows).wait_send()

        copy = to_source(0, peer, peer, peer)
        copy.wait_send()
        copy.wait_recv()
        return 0

    lax.fori_loop(1, devices, finish, 0)

    def finish_partner(row, _):
        for k in range(1, n_grp):
            g = lax.rem(group_index + k, n_grp)
            copy = to_partner(row, g, g)
            copy.wait_send()
            copy.wait_recv()
        return 0

    lax.fori_loop(0, n_scan, finish_partner, 0)


def regroup(parts, width):
    groups = len(parts)
    lane = lax.broadcasted_iota(jnp.int32, parts[0].shape, 1) // width
    out = []
    for b in range(groups):
        total = parts[b]
        for g in range(groups):
            if g != b:
                total = jnp.where(lane == g, pltpu.roll(parts[g], (g - b) * width % LANES, 1), total)
        out.append(total)
    return out


def assemble_kernel(n_grp, width, by_source, by_partner, hessian, gradient, total):
    rows, columns = hessian.shape[2], hessian.shape[3]
    grad_rows = gradient.shape[0]
    packed_rows = by_source.shape[1]
    groups = LANES // width
    scan_index, group_index = lax.axis_index("scan"), lax.axis_index("grp")
    cells = rows * columns
    total[...] = jnp.zeros_like(total)
    step = 2 * groups

    def place(ids, first, size):
        local = ids - first
        return local, (local >= 0) & (local < size)

    def add(read, sign):
        def body(i, _):
            turned = []
            for half in range(2):
                parts = [read(i * step + half * groups + g) for g in range(groups)]
                turned.append(jnp.concatenate(regroup(parts, width), axis=0))
            values = jnp.concatenate(turned, axis=1)
            source, partner = values[27:28, :].astype(jnp.int32), values[28:29, :].astype(jnp.int32)
            own, other = (source, partner) if sign > 0 else (partner, source)
            row, row_ok = place(own, scan_index * rows, rows)
            plus, plus_ok = place(own, group_index * columns, columns)
            minus, minus_ok = place(other, group_index * columns, columns)
            plus = jnp.where(row_ok & plus_ok, row * columns + plus, -1)
            minus = jnp.where(row_ok & minus_ok, row * columns + minus, -1)
            grad, grad_ok = place(row, group_index * grad_rows, grad_rows)
            grad = jnp.where(row_ok & grad_ok, grad, -1)
            cell = lax.broadcasted_iota(jnp.int32, (cells, 2 * LANES), 0)
            chosen = jnp.where(cell == plus, 1.0, jnp.where(cell == minus, -1.0, 0.0))
            short = lax.broadcasted_iota(jnp.int32, (16, 2 * LANES), 0)
            chosen_grad = jnp.where(short == grad, float(sign), 0.0)
            matrix = jnp.concatenate([chosen, chosen_grad], axis=0).astype(jnp.bfloat16)
            high = values.astype(jnp.bfloat16)
            low = (values - high.astype(jnp.float32)).astype(jnp.bfloat16)
            both = jnp.concatenate([high, low], axis=0)
            total[...] += lax.dot_general(
                matrix, both, (((1,), (1,)), ((), ())), preferred_element_type=jnp.float32
            )
            return 0

        return body

    blocks = by_source.shape[0]
    n_scan = by_partner.shape[1]
    lax.fori_loop(0, blocks // step, add(lambda k: by_source[k], 1), 0)
    lax.fori_loop(0, blocks // step, add(lambda k: by_partner[k // n_scan, k % n_scan], -1), 0)
    result = total[:, 0:VALUES] + total[:, VALUES : 2 * VALUES]
    turned = result[0:cells, :].T
    where = {pair: q for q, pair in enumerate(PAIRS)}
    for i in range(6):
        ids = [where[min(i, j), max(i, j)] for j in range(6)]
        band = jnp.concatenate([turned[q : q + 1, :] for q in ids], axis=0)
        for r in range(rows):
            hessian[i, :, r, :] = band[:, r * columns : (r + 1) * columns]
    gradient[...] = result[cells : cells + grad_rows, 21:27]


def local(samples, point_count, corr_scan, corr_tile, corr_src):
    f32, i32 = jnp.float32, jnp.int32
    scan_local = samples.shape[0]
    request_count = scan_local * corr_scan.shape[1]
    n_scan, n_grp = lax.axis_size("scan"), lax.axis_size("grp")
    devices = n_scan * n_grp
    cap = 2 * request_count // devices
    width = n_grp * cap
    packed_rows = VALUES * width // LANES
    columns = scan_local * n_scan // n_grp
    grad_rows = scan_local // n_grp
    shape = jax.ShapeDtypeStruct
    dma = pltpu.SemaphoreType.DMA

    tiles = samples.transpose(0, 2, 1, 3)
    data, meta = pl.pallas_call(
        functools.partial(pack_kernel, cap, n_grp),
        out_shape=(shape((devices * cap * 4, LANES), f32), shape((devices, 1, LANES), i32)),
        in_specs=[VMEM, SMEM, SMEM, SMEM, VMEM],
        out_specs=(VMEM, SMEM),
        scratch_shapes=[pltpu.SMEM((devices,), i32)],
    )(tiles, point_count, corr_scan, corr_tile, corr_src)

    by_source, by_partner = pl.pallas_call(
        functools.partial(exchange_kernel, cap, n_grp),
        out_shape=(
            shape((devices, packed_rows, LANES), f32),
            shape((n_grp, n_scan, packed_rows, LANES), f32),
        ),
        in_specs=[VMEM, SMEM, VMEM, VMEM],
        out_specs=(VMEM, VMEM),
        scratch_shapes=[
            pltpu.VMEM(data.shape, f32),
            pltpu.VMEM(meta.shape, i32),
            pltpu.SMEM(meta.shape, i32),
            pltpu.VMEM((9, 16, LANES), f32),
            pltpu.VMEM((LANES, LANES), f32),
            pltpu.VMEM((n_scan, packed_rows, LANES), f32),
        ]
        + [dma((devices,))] * 6
        + [dma((n_grp, n_scan))] * 2
        + [dma((3,))],
        compiler_params=pltpu.CompilerParams(collective_id=0, has_side_effects=True),
    )(tiles, point_count, data, meta)

    hessian, gradient = pl.pallas_call(
        functools.partial(assemble_kernel, n_grp, width),
        out_shape=(shape((6, 6, scan_local, columns), f32), shape((grad_rows, 6), f32)),
        in_specs=[VMEM, VMEM],
        out_specs=(VMEM, VMEM),
        scratch_shapes=[pltpu.VMEM((scan_local * columns + 16, 2 * VALUES), f32)],
    )(by_source, by_partner)
    return hessian.transpose(2, 0, 1, 3), gradient


def solution(mesh):
    placed = (
        P("scan", "grp", None, None),
        P("scan"),
        P("scan", "grp"),
        P("scan", "grp"),
        P("scan", "grp", None),
    )
    return jax.shard_map(
        local,
        mesh=mesh,
        in_specs=placed,
        out_specs=(P("scan", None, None, "grp"), P(("scan", "grp"), None)),
        check_vma=False,
    )
```
